8 devices in a mesh: dp: 2 (over z, y), cp: 4 (over x, core).
Axes of the slice: x: 2, y: 2, z: 1, core: 2. Of those that a mesh axis runs over, the one named last changes fastest.
Arguments:
- hidden: bfloat16 [8192, 4096], P(('dp', 'cp')), parts along dimension 0
- seg_id: int32 [8192], P(('dp', 'cp')), parts along dimension 0
- doc_pos: int32 [8192], P(('dp', 'cp')), parts along dimension 0
- norm_gain: bfloat16 [4096], replicated
- w_qkv: bfloat16 [4096, 4608], replicated
- b_qkv: bfloat16 [4608], replicated
- w_out: bfloat16 [4096, 4096], replicated
- grad_out: bfloat16 [8192, 4096], P(('dp', 'cp')), parts along dimension 0
Outputs:
- output 1: bfloat16 [8192, 4096], P(('dp', 'cp')), parts along dimension 0
- output 2: bfloat16 [8192, 4096], P(('dp', 'cp')), parts along dimension 0
- output 3: float32 [8192], P('dp'), parts along dimension 0
- output 4: float32 [8192, 4608], P('dp'), parts along dimension 0
- output 5: float32 [9216], P('dp'), parts along dimension 0
- output 6: float32 [8192, 4096], P('dp'), parts along dimension 0
There are 2 independent parts. The reference program is written for one: setup_inputs(seed, part) draws one part's arguments, and reference() takes and returns one part's arrays. A program takes and returns all parts, laid end to end along the dimension named above; an argument that names none is the same for every part.
All inputs are finite; a program needn't handle non-finite values.
Results may differ from the reference program's by a relative error of at most 0.0186529.
Values are sent between devices in bfloat16 or wider.
A program may use at most 1 GiB of HBM per device.

```python
import jax
import jax.numpy as jnp
from jax import lax

D = 4096
HEADS = 32
GROUPS = 2
HEAD = 128
SEQ = 4096
DOCS = 4
BLOCK = 128

ROT_DIMS = HEAD // 2
REP_HEADS = HEADS // GROUPS
ATT_WIDTH = HEADS * HEAD
KV_WIDTH = GROUPS * HEAD
QKV_WIDTH = ATT_WIDTH + 2 * KV_WIDTH
ROPE_BASE = 5000000.0
EPS_NORM = 1e-5
NEG_BIG = -1e30


def draw_documents(doc_key):
    cut_points = jax.random.permutation(doc_key, SEQ - 1)[: DOCS - 1] + 1
    start_flag = jnp.zeros((SEQ,), jnp.int32).at[cut_points].set(1)
    seg_id = jnp.cumsum(start_flag).astype(jnp.int32)
    tok_index = jnp.arange(SEQ, dtype=jnp.int32)
    doc_start = lax.cummax(jnp.where(start_flag > 0, tok_index, 0), axis=0)
    return seg_id, (tok_index - doc_start).astype(jnp.int32)


def setup_inputs(seed: int = 0, part: int = 0) -> dict:
    root_key = jax.random.key(seed)
    key_gain, key_wqkv, key_bqkv, key_wout = jax.random.split(root_key, 4)
    part_key = jax.random.fold_in(root_key, part)
    key_x, key_doc, key_dy = jax.random.split(part_key, 3)
    seg_id, doc_pos = draw_documents(key_doc)
    hidden = jax.random.normal(key_x, (SEQ, D), jnp.float32)
    norm_gain = 1.0 + 0.3 * jax.random.normal(key_gain, (D,), jnp.float32)
    w_qkv = 1.5 * D ** -0.5 * jax.random.normal(key_wqkv, (D, QKV_WIDTH), jnp.float32)
    b_qkv = 0.5 * jax.random.normal(key_bqkv, (QKV_WIDTH,), jnp.float32)
    w_out = ATT_WIDTH ** -0.5 * jax.random.normal(key_wout, (ATT_WIDTH, D), jnp.float32)
    grad_out = jax.random.normal(key_dy, (SEQ, D), jnp.float32)
    return {
        'hidden': hidden.astype(jnp.bfloat16),
        'seg_id': seg_id,
        'doc_pos': doc_pos,
        'norm_gain': norm_gain.astype(jnp.bfloat16),
        'w_qkv': w_qkv.astype(jnp.bfloat16),
        'b_qkv': b_qkv.astype(jnp.bfloat16),
        'w_out': w_out.astype(jnp.bfloat16),
        'grad_out': grad_out.astype(jnp.bfloat16),
    }


def rotate(values, cos_ang, sin_ang):
    rot_pairs = values[..., :ROT_DIMS].reshape(values.shape[:-1] + (ROT_DIMS // 2, 2))
    even_part = rot_pairs[..., 0]
    odd_part = rot_pairs[..., 1]
    turned = jnp.stack([even_part * cos_ang - odd_part * sin_ang, odd_part * cos_ang + even_part * sin_ang], axis=-1)
    return jnp.concatenate([turned.reshape(values.shape[:-1] + (ROT_DIMS,)), values[..., ROT_DIMS:]], axis=-1)


def attention_core(q_rot, k_rot, v_val, seg_id):
    n_blocks = SEQ // BLOCK
    scale = HEAD ** -0.5
    q_blocks = q_rot.reshape(n_blocks, BLOCK, GROUPS, REP_HEADS, HEAD)
    k_blocks = k_rot.reshape(n_blocks, BLOCK, GROUPS, HEAD)
    v_blocks = v_val.reshape(n_blocks, BLOCK, GROUPS, HEAD)
    seg_blocks = seg_id.reshape(n_blocks, BLOCK)
    offsets = jnp.arange(BLOCK)

    def query_block(blk_args):
        q_idx, q_blk, seg_q = blk_args

        def key_step(loop_vals, key_args):
            k_idx, k_blk, v_blk, seg_k = key_args
            vis_mask = (seg_q[:, None] == seg_k[None, :]) & (k_idx * BLOCK + offsets[None, :] <= q_idx * BLOCK + offsets[:, None])

            def advance(run_state):
                m_run, l_run, acc_sum = run_state
                scores = jnp.einsum('qgrd,kgd->grqk', q_blk, k_blk) * scale
                scores = jnp.where(vis_mask, scores, NEG_BIG)
                m_new = jnp.maximum(m_run, jnp.max(scores, axis=-1))
                p_mat = jnp.where(vis_mask, jnp.exp(scores - m_new[..., None]), 0.0)
                rescale = jnp.exp(m_run - m_new)
                return (m_new, l_run * rescale + jnp.sum(p_mat, axis=-1), acc_sum * rescale[..., None] + jnp.einsum('grqk,kgd->grqd', p_mat, v_blk))

            return lax.cond(jnp.any(vis_mask), advance, lambda run_state: run_state, loop_vals), None

        init_state = (
            jnp.full((GROUPS, REP_HEADS, BLOCK), NEG_BIG, jnp.float32),
            jnp.zeros((GROUPS, REP_HEADS, BLOCK), jnp.float32),
            jnp.zeros((GROUPS, REP_HEADS, BLOCK, HEAD), jnp.float32),
        )
        final_state, _ = lax.scan(jax.checkpoint(key_step), init_state, (jnp.arange(n_blocks), k_blocks, v_blocks, seg_blocks))
        return final_state[2] / final_state[1][..., None]

    context = lax.map(jax.checkpoint(query_block), (jnp.arange(n_blocks), q_blocks, seg_blocks))
    return context.transpose(0, 3, 1, 2, 4).reshape(SEQ, GROUPS, REP_HEADS, HEAD)


def reference(hidden, seg_id, doc_pos, norm_gain, w_qkv, b_qkv, w_out, grad_out):
    hid_f32 = hidden.astype(jnp.float32)
    inv_rms = lax.rsqrt(jnp.mean(hid_f32 * hid_f32, axis=-1, keepdims=True) + EPS_NORM)
    x_hat = hid_f32 * inv_rms
    gain_f32 = norm_gain.astype(jnp.float32)
    normed = (x_hat * gain_f32).astype(jnp.bfloat16)
    qkv_out = (jnp.dot(normed, w_qkv, preferred_element_type=jnp.float32) + b_qkv.astype(jnp.float32)).astype(jnp.bfloat16)
    inv_freq = ROPE_BASE ** (-jnp.arange(0, ROT_DIMS, 2).astype(jnp.float32) / ROT_DIMS)
    angles = doc_pos.astype(jnp.float32)[:, None] * inv_freq[None, :]
    cos_q = jnp.cos(angles)[:, None, None, :]
    sin_q = jnp.sin(angles)[:, None, None, :]
    cos_k = jnp.cos(angles)[:, None, :]
    sin_k = jnp.sin(angles)[:, None, :]
    q_rot = rotate(qkv_out[:, :ATT_WIDTH].astype(jnp.float32).reshape(SEQ, GROUPS, REP_HEADS, HEAD), cos_q, sin_q).astype(jnp.bfloat16)
    k_rot = rotate(qkv_out[:, ATT_WIDTH:ATT_WIDTH + KV_WIDTH].astype(jnp.float32).reshape(SEQ, GROUPS, HEAD), cos_k, sin_k).astype(jnp.bfloat16)
    v_val = qkv_out[:, ATT_WIDTH + KV_WIDTH:].reshape(SEQ, GROUPS, HEAD)
    ctx_f32, attn_vjp = jax.vjp(
        lambda q_in, k_in, v_in: attention_core(q_in, k_in, v_in, seg_id),
        q_rot.astype(jnp.float32), k_rot.astype(jnp.float32), v_val.astype(jnp.float32))
    context = ctx_f32.astype(jnp.bfloat16).reshape(SEQ, ATT_WIDTH)
    y_out = (hid_f32 + jnp.dot(context, w_out, preferred_element_type=jnp.float32)).astype(jnp.bfloat16)
    grad_ctx = jnp.dot(grad_out, w_out.T, preferred_element_type=jnp.float32).astype(jnp.bfloat16)
    grad_wout = jnp.dot(context.T, grad_out, preferred_element_type=jnp.float32)
    d_query, d_key, d_value = attn_vjp(grad_ctx.astype(jnp.float32).reshape(SEQ, GROUPS, REP_HEADS, HEAD))
    grad_qkv = jnp.concatenate([
        rotate(d_query, cos_q, -sin_q).reshape(SEQ, ATT_WIDTH),
        rotate(d_key, cos_k, -sin_k).reshape(SEQ, KV_WIDTH),
        d_value.reshape(SEQ, KV_WIDTH)], axis=1).astype(jnp.bfloat16)
    grad_bqkv = jnp.sum(grad_qkv.astype(jnp.float32), axis=0)
    grad_wqkv = jnp.dot(normed.T, grad_qkv, preferred_element_type=jnp.float32)
    grad_normed = jnp.dot(grad_qkv, w_qkv.T, preferred_element_type=jnp.float32)
    grad_gain = jnp.sum(grad_normed * x_hat, axis=0)
    scaled = grad_normed * gain_f32
    grad_hidden = (grad_out.astype(jnp.float32) + inv_rms * (scaled - x_hat * jnp.mean(scaled * x_hat, axis=-1, keepdims=True))).astype(jnp.bfloat16)
    return (y_out, grad_hidden, grad_gain, grad_wqkv, grad_bqkv, grad_wout)
```

```python
import functools

import jax
import jax.numpy as jnp
from jax import lax
from jax.experimental import pallas as pl
from jax.experimental.pallas import tpu as pltpu
from jax.sharding import PartitionSpec as P

HEAD_DIM = 128
ROT_DIMS = 64
ROPE_BASE = 5000000.0
EPS_NORM = 1e-5
NEG_BIG = -1e30
LOG2E = 1.4426950408889634
BQ = 256
BK = 256
VMEM_LIMIT = 60 * 1024 * 1024


NT = (((1,), (1,)), ((), ()))
NN = (((1,), (0,)), ((), ()))
TN = (((0,), (0,)), ((), ()))


def dotf(a, b, dims):
    return lax.dot_general(a, b, dims, preferred_element_type=jnp.float32)


def pair_swap(values):
    lane = lax.broadcasted_iota(jnp.int32, values.shape, 1)
    return jnp.where(lane % 2 == 0, pltpu.roll(values, HEAD_DIM - 1, 1), pltpu.roll(values, 1, 1))


def load_rotated(q_ref, cos_ref, sin_ref, qs_ref, n_heads):
    cos_t = cos_ref[...]
    sin_t = sin_ref[...]
    for h in range(n_heads):
        val = q_ref[:, h * HEAD_DIM:(h + 1) * HEAD_DIM].astype(jnp.float32)
        qs_ref[h * BQ:(h + 1) * BQ, :] = (val * cos_t + pair_swap(val) * sin_t).astype(jnp.bfloat16)


def visible(start_row, kv, q_base):
    k_idx = kv * BK + lax.broadcasted_iota(jnp.int32, (BK, BQ), 0)
    q_idx = q_base + lax.broadcasted_iota(jnp.int32, (BK, BQ), 1)
    return (k_idx >= start_row) & (k_idx <= q_idx)


def mask_heads(s_t, start_row, kv, q_base, n_heads):
    vis = visible(start_row, kv, q_base)
    return jnp.concatenate([jnp.where(vis, s_t[:, h * BQ:(h + 1) * BQ], NEG_BIG) for h in range(n_heads)], axis=1)


def fwd_kernel(n_heads, sc_ref, q_ref, cos_ref, sin_ref, start_ref, k_ref, vt_ref,
               ctx_ref, lse_ref, qs_ref, acc_ref):
    i = pl.program_id(0)
    q_base = sc_ref[0] + i * BQ
    lo = sc_ref[1 + 2 * i]
    full_lo = sc_ref[2 + 2 * i]
    diag = q_base // BK
    scale = HEAD_DIM ** -0.5 * LOG2E
    load_rotated(q_ref, cos_ref, sin_ref, qs_ref, n_heads)
    start_row = start_ref[...]
    acc_ref[...] = jnp.zeros_like(acc_ref)

    def step(masked, kv, carry):
        m_run, l_run = carry
        k_off = pl.multiple_of(kv * BK, BK)
        s_t = dotf(k_ref[pl.ds(k_off, BK), :], qs_ref[...], NT) * scale
        if masked:
            s_t = mask_heads(s_t, start_row, kv, q_base, n_heads)
        m_new = jnp.maximum(m_run, jnp.max(s_t, axis=0, keepdims=True))
        p_t = jnp.exp2(s_t - m_new)
        rescale = jnp.exp2(m_run - m_new)
        l_new = l_run * rescale + jnp.sum(p_t, axis=0, keepdims=True)
        acc_ref[...] = acc_ref[...] * rescale + dotf(vt_ref[:, pl.ds(k_off, BK)], p_t.astype(jnp.bfloat16), NN)
        return m_new, l_new

    carry = (jnp.full((1, n_heads * BQ), NEG_BIG, jnp.float32), jnp.zeros((1, n_heads * BQ), jnp.float32))
    carry = lax.fori_loop(lo, full_lo, functools.partial(step, True), carry)
    carry = lax.fori_loop(full_lo, diag, functools.partial(step, False), carry)
    m_run, l_run = step(True, diag, carry)
    lse = m_run + jnp.log2(l_run)
    for h in range(n_heads):
        span = slice(h * BQ, (h + 1) * BQ)
        o_t = acc_ref[:, span] / l_run[:, span]
        ctx_ref[:, h * HEAD_DIM:(h + 1) * HEAD_DIM] = o_t.T.astype(jnp.bfloat16)
        lse_ref[h:h + 1, :] = lse[:, span]


def bwd_kernel(n_heads, sc_ref, q_ref, do_ref, ctx_ref, lse_ref, cos_ref, sin_ref, start_ref,
               k_ref, kt_ref, v_ref, dq_ref, dk_ref, dv_ref, qs_ref, ds_ref, rd_ref, dqt_ref):
    i = pl.program_id(0)
    q_base = sc_ref[0] + i * BQ
    lo = sc_ref[1 + 2 * i]
    full_lo = sc_ref[2 + 2 * i]
    diag = q_base // BK
    factor = HEAD_DIM ** -0.5
    scale = factor * LOG2E

    @pl.when(i == 0)
    def _():
        dk_ref[...] = jnp.zeros_like(dk_ref)
        dv_ref[...] = jnp.zeros_like(dv_ref)

    load_rotated(q_ref, cos_ref, sin_ref, qs_ref, n_heads)
    for h in range(n_heads):
        cols = slice(h * HEAD_DIM, (h + 1) * HEAD_DIM)
        do_h = do_ref[:, cols]
        ds_ref[h * BQ:(h + 1) * BQ, :] = do_h
        prod = do_h.astype(jnp.float32) * ctx_ref[:, cols].astype(jnp.float32)
        span = slice(h * BQ, (h + 1) * BQ)
        rd_ref[0:1, span] = jnp.sum(prod.T, axis=0, keepdims=True)
        rd_ref[1:2, span] = lse_ref[h:h + 1, :]
    start_row = start_ref[...]
    cos_t = cos_ref[...]
    sin_t = sin_ref[...]
    dqt_ref[...] = jnp.zeros_like(dqt_ref)
    row_dot = rd_ref[0:1, :]
    log_norm = rd_ref[1:2, :]

    def step(masked, kv, _):
        k_off = pl.multiple_of(kv * BK, BK)
        keys = pl.ds(k_off, BK)
        s_t = dotf(k_ref[keys, :], qs_ref[...], NT) * scale
        if masked:
            s_t = mask_heads(s_t, start_row, kv, q_base, n_heads)
        p_t = jnp.exp2(s_t - log_norm)
        g_t = (p_t * (dotf(v_ref[keys, :], ds_ref[...], NT) - row_dot)).astype(jnp.bfloat16)
        dqt_ref[...] += dotf(kt_ref[:, keys], g_t, NN)
        dv_ref[keys, :] += dotf(p_t.astype(jnp.bfloat16), ds_ref[...], NN)
        dk_ref[keys, :] += dotf(g_t, qs_ref[...], NN)
        return 0

    lax.fori_loop(lo, full_lo, functools.partial(step, True), 0)
    lax.fori_loop(full_lo, diag, functools.partial(step, False), 0)
    step(True, diag, 0)
    for h in range(n_heads):
        dq_h = dqt_ref[:, h * BQ:(h + 1) * BQ].T * factor
        dq_ref[:, h * HEAD_DIM:(h + 1) * HEAD_DIM] = (dq_h * cos_t - pair_swap(dq_h) * sin_t).astype(jnp.bfloat16)


def attn_cost(n_rows, width, n_dots):
    return pl.CostEstimate(flops=int(n_dots * 4 * n_rows * 1400 * width), bytes_accessed=3 * n_rows * width * 2,
                           transcendentals=0)


def attention_fwd(scal, q_pre, cos_t, sin_t, start_row, k_all, vt_all):
    n_rows, width = q_pre.shape
    n_heads = width // HEAD_DIM
    n_keys = k_all.shape[0]
    row_blk = lambda i, sc: (i, 0)
    lane_blk = lambda i, sc: (0, i)
    whole = lambda i, sc: (0, 0)
    return pl.pallas_call(
        functools.partial(fwd_kernel, n_heads),
        grid_spec=pltpu.PrefetchScalarGridSpec(
            num_scalar_prefetch=1, grid=(n_rows // BQ,),
            in_specs=[pl.BlockSpec((BQ, width), row_blk), pl.BlockSpec((BQ, HEAD_DIM), row_blk),
                      pl.BlockSpec((BQ, HEAD_DIM), row_blk), pl.BlockSpec((1, BQ), lane_blk),
                      pl.BlockSpec((n_keys, HEAD_DIM), whole), pl.BlockSpec((HEAD_DIM, n_keys), whole)],
            out_specs=[pl.BlockSpec((BQ, width), row_blk), pl.BlockSpec((n_heads, BQ), lane_blk)],
            scratch_shapes=[pltpu.VMEM((n_heads * BQ, HEAD_DIM), jnp.bfloat16),
                            pltpu.VMEM((HEAD_DIM, n_heads * BQ), jnp.float32)]),
        out_shape=[jax.ShapeDtypeStruct((n_rows, width), jnp.bfloat16), jax.ShapeDtypeStruct((n_heads, n_rows), jnp.float32)],
        compiler_params=pltpu.CompilerParams(dimension_semantics=("arbitrary",), vmem_limit_bytes=VMEM_LIMIT),
        cost_estimate=attn_cost(n_rows, width, 1), name="attn_fwd",
    )(scal, q_pre, cos_t, sin_t, start_row, k_all, vt_all)


def attention_bwd(scal, q_pre, grad_ctx, ctx, lse, cos_t, sin_t, start_row, k_all, kt_all, v_all):
    n_rows, width = q_pre.shape
    n_heads = width // HEAD_DIM
    n_keys = k_all.shape[0]
    row_blk = lambda i, sc: (i, 0)
    lane_blk = lambda i, sc: (0, i)
    whole = lambda i, sc: (0, 0)
    wide = pl.BlockSpec((BQ, width), row_blk)
    kv_spec = pl.BlockSpec((n_keys, HEAD_DIM), whole)
    return pl.pallas_call(
        functools.partial(bwd_kernel, n_heads),
        grid_spec=pltpu.PrefetchScalarGridSpec(
            num_scalar_prefetch=1, grid=(n_rows // BQ,),
            in_specs=[wide, wide, wide, pl.BlockSpec((n_heads, BQ), lane_blk), pl.BlockSpec((BQ, HEAD_DIM), row_blk),
                      pl.BlockSpec((BQ, HEAD_DIM), row_blk), pl.BlockSpec((1, BQ), lane_blk),
                      kv_spec, pl.BlockSpec((HEAD_DIM, n_keys), whole), kv_spec],
            out_specs=[wide, kv_spec, kv_spec],
            scratch_shapes=[pltpu.VMEM((n_heads * BQ, HEAD_DIM), jnp.bfloat16),
                            pltpu.VMEM((n_heads * BQ, HEAD_DIM), jnp.bfloat16),
                            pltpu.VMEM((2, n_heads * BQ), jnp.float32),
                            pltpu.VMEM((HEAD_DIM, n_heads * BQ), jnp.float32)]),
        out_shape=[jax.ShapeDtypeStruct((n_rows, width), jnp.bfloat16)] + [jax.ShapeDtypeStruct((n_keys, HEAD_DIM), jnp.float32)] * 2,
        compiler_params=pltpu.CompilerParams(dimension_semantics=("arbitrary",), vmem_limit_bytes=VMEM_LIMIT),
        cost_estimate=attn_cost(n_rows, width, 2.5), name="attn_bwd",
    )(scal, q_pre, grad_ctx, ctx, lse, cos_t, sin_t, start_row, k_all, kt_all, v_all)


def wgrad_kernel(col_step, n_prev, n_out, sc_ref, a0_ref, a1_ref, b0_ref, b1_ref, *refs):
    out_refs = refs[-n_out:]
    width = out_refs[0].shape[1]

    def cols(j, _):
        span = pl.ds(pl.multiple_of(j * col_step, col_step), col_step)
        total = dotf(a0_ref[...], b0_ref[:, span], TN) + dotf(a1_ref[...], b1_ref[:, span], TN)
        if n_prev:
            total = refs[0][:, span] + total
        for out in out_refs:
            out[:, span] = total
        return 0

    lax.fori_loop(0, width // col_step, cols, 0)


def weight_grad(a_pair, b_pair, prev, place, full, col0, n_dim, bm, bn, col_step):
    n_tok, m_dim = a_pair[0].shape
    blk0 = col0 // bn
    a_spec = pl.BlockSpec((n_tok, bm), lambda n, m, sc: (0, m))
    b_spec = pl.BlockSpec((n_tok, bn), lambda n, m, sc: (0, n + blk0))
    in_specs = [a_spec] * 2 + [b_spec] * 2
    args = [*a_pair, *b_pair]
    if prev is not None:
        in_specs.append(pl.BlockSpec((bm, bn), lambda n, m, sc: (m, n + blk0)))
        args.append(prev)
    out_specs = [pl.BlockSpec((bm, bn), lambda n, m, sc: (m, n))]
    out_shape = [jax.ShapeDtypeStruct((m_dim, n_dim), jnp.float32)]
    aliases = {}
    if full is not None:
        shape = full if isinstance(full, tuple) else full.shape
        out_specs.append(pl.BlockSpec((bm, bn), lambda n, m, sc: (sc[0] + m, sc[1] + n)))
        out_shape.append(jax.ShapeDtypeStruct(shape, jnp.float32))
        if not isinstance(full, tuple):
            in_specs.append(pl.BlockSpec(memory_space=pl.ANY))
            args.append(full)
            aliases = {len(args): 1}
    return pl.pallas_call(
        functools.partial(wgrad_kernel, col_step, prev is not None, len(out_shape)),
        grid_spec=pltpu.PrefetchScalarGridSpec(num_scalar_prefetch=1, grid=(n_dim // bn, m_dim // bm),
                                               in_specs=in_specs, out_specs=out_specs),
        out_shape=out_shape, input_output_aliases=aliases,
        compiler_params=pltpu.CompilerParams(dimension_semantics=("arbitrary", "arbitrary"), vmem_limit_bytes=VMEM_LIMIT),
        cost_estimate=pl.CostEstimate(flops=4 * n_tok * m_dim * n_dim, transcendentals=0,
                                      bytes_accessed=m_dim * n_dim * 8 + 4 * n_tok * (m_dim + n_dim)),
    )(place, *args)


def place_kernel(sc_ref, src_ref, full_ref, out_ref):
    out_ref[...] = src_ref[...]


def place_block(full, block, place, bm, bn):
    m_dim, n_dim = block.shape
    return pl.pallas_call(
        place_kernel,
        grid_spec=pltpu.PrefetchScalarGridSpec(
            num_scalar_prefetch=1, grid=(m_dim // bm, n_dim // bn),
            in_specs=[pl.BlockSpec((bm, bn), lambda m, n, sc: (m, n)), pl.BlockSpec(memory_space=pl.ANY)],
            out_specs=pl.BlockSpec((bm, bn), lambda m, n, sc: (sc[0] + m, sc[1] + n))),
        out_shape=jax.ShapeDtypeStruct(full.shape, full.dtype),
        input_output_aliases={2: 0},
        compiler_params=pltpu.CompilerParams(dimension_semantics=("arbitrary", "arbitrary"), vmem_limit_bytes=VMEM_LIMIT),
        cost_estimate=pl.CostEstimate(flops=0, transcendentals=0, bytes_accessed=8 * m_dim * n_dim),
    )(place, block, full)


def swap_lanes(values):
    lane = lax.broadcasted_iota(jnp.int32, values.shape, values.ndim - 1)
    return jnp.where(lane % 2 == 0, jnp.roll(values, -1, axis=-1), jnp.roll(values, 1, axis=-1))


def solution(mesh):
    core_swap = [(0, 1), (1, 0), (2, 3), (3, 2)]
    chip_swap = [(0, 2), (2, 0), (1, 3), (3, 1)]

    def to_core(val):
        return lax.ppermute(val, 'cp', core_swap)

    def to_chip(val):
        return lax.ppermute(val, 'cp', chip_swap)

    def to_later(val):
        return lax.ppermute(val, 'cp', [(0, 2), (1, 3)])

    def to_earlier(val):
        return lax.ppermute(val, 'cp', [(2, 0), (3, 1)])

    def layer(hidden, seg_id, doc_pos, norm_gain, w_qkv, b_qkv, w_out, grad_out):
        n_rows, hid_width = hidden.shape
        att_width = w_out.shape[0]
        half = att_width // 2
        idx = lax.axis_index('cp')
        core = idx % 2
        chip = idx // 2
        chunk_ids = (idx, idx ^ 1, idx ^ 2, idx ^ 3)

        pos_all = lax.all_gather(doc_pos, 'cp', axis=0, tiled=True)
        hidden, grad_out, pos_all = lax.optimization_barrier((hidden, grad_out, pos_all))

        go_rm = to_chip(grad_out)
        hid_f32 = hidden.astype(jnp.float32)
        inv_rms = lax.rsqrt(jnp.mean(hid_f32 * hid_f32, axis=-1, keepdims=True) + EPS_NORM)
        x_hat = hid_f32 * inv_rms
        gain_f32 = norm_gain.astype(jnp.float32)
        normed = (x_hat * gain_f32).astype(jnp.bfloat16)
        normed_p = to_core(normed)
        go_p = to_core(grad_out)

        n_seq = pos_all.shape[0]
        starts = jnp.arange(n_seq, dtype=jnp.int32) - pos_all
        lane = jnp.arange(HEAD_DIM)
        exponent = -((lane // 2) * 2).astype(jnp.float32) / ROT_DIMS
        inv_freq = ROPE_BASE ** exponent
        angles = pos_all.astype(jnp.float32)[:, None] * inv_freq[None, :]
        turned = (lane < ROT_DIMS)[None, :]
        cos_all = jnp.where(turned, jnp.cos(angles), 1.0)
        sin_all = jnp.where(turned, jnp.sin(angles) * jnp.where(lane % 2 == 0, -1.0, 1.0)[None, :], 0.0)

        def chunk_of(arr, g, axis=0):
            return lax.dynamic_slice_in_dim(arr, g * n_rows, n_rows, axis)

        cos_c = [chunk_of(cos_all, g) for g in chunk_ids]
        sin_c = [chunk_of(sin_all, g) for g in chunk_ids]
        start_c = [chunk_of(starts, g) for g in chunk_ids]
        scal_c = []
        for g, st in zip(chunk_ids, start_c):
            diag = (g * n_rows) // BK + jnp.arange(n_rows // BQ, dtype=jnp.int32) * (BQ // BK)
            lo = st[::BQ] // BK
            full_lo = jnp.minimum((st[BQ - 1::BQ] + BK - 1) // BK, diag)
            lo = jnp.minimum(lo, full_lo)
            scal_c.append(jnp.concatenate([(g * n_rows)[None], jnp.stack([lo, full_lo], axis=1).reshape(-1)]).astype(jnp.int32))
        row_c = [st[None, :] for st in start_c]

        wq = lax.dynamic_slice(w_qkv, (0, core * half), (hid_width, half))
        wk = lax.dynamic_slice(w_qkv, (0, att_width + core * HEAD_DIM), (hid_width, HEAD_DIM))
        wv = lax.dynamic_slice(w_qkv, (0, att_width + (2 + core) * HEAD_DIM), (hid_width, HEAD_DIM))
        wkv = jnp.concatenate([wk, wv], axis=1)
        b_f32 = b_qkv.astype(jnp.float32)
        bq = lax.dynamic_slice(b_f32, (core * half,), (half,))
        bkv = jnp.concatenate([lax.dynamic_slice(b_f32, (att_width + core * HEAD_DIM,), (HEAD_DIM,)),
                               lax.dynamic_slice(b_f32, (att_width + (2 + core) * HEAD_DIM,), (HEAD_DIM,))])
        wo = lax.dynamic_slice(w_out, (core * half, 0), (half, hid_width))

        def project(act, wgt, bias):
            return (jnp.dot(act, wgt, preferred_element_type=jnp.float32) + bias).astype(jnp.bfloat16)

        def project_kv(act, i):
            kv = project(act, wkv, bkv)
            k_f32 = kv[:, :HEAD_DIM].astype(jnp.float32)
            k_rot = (k_f32 * cos_c[i] + swap_lanes(k_f32) * sin_c[i]).astype(jnp.bfloat16)
            return jnp.concatenate([k_rot, kv[:, HEAD_DIM:]], axis=1)

        kv_m = project_kv(normed, 0)
        kv_rm = to_later(kv_m)
        kv_p = project_kv(normed_p, 1)
        kv_rp = to_later(kv_p)
        norm_sent, kv_m, kv_p = lax.optimization_barrier((normed, kv_m, kv_p))
        norm_rm = to_chip(norm_sent)
        q_m = project(normed, wq, bq)
        q_p = project(normed_p, wq, bq)

        def grad_context(go):
            return lax.dot_general(go, wo, NT, preferred_element_type=jnp.float32).astype(jnp.bfloat16)

        gctx_m, gctx_p = grad_context(grad_out), grad_context(go_p)
        kv_rm, kv_rp, q_m, q_p, gctx_m, gctx_p = lax.optimization_barrier((kv_rm, kv_rp, q_m, q_p, gctx_m, gctx_p))
        kv_all = jnp.zeros((n_seq, 2 * HEAD_DIM), jnp.bfloat16)
        for g, kv in zip(chunk_ids, (kv_m, kv_p, kv_rm, kv_rp)):
            kv_all = lax.dynamic_update_slice(kv_all, kv, (g * n_rows, 0))
        k_all, v_all = kv_all[:, :HEAD_DIM], kv_all[:, HEAD_DIM:]
        kt_all, vt_all = k_all.T, v_all.T

        def forward(i, q):
            return attention_fwd(scal_c[i], q, cos_c[i], sin_c[i], row_c[i], k_all, vt_all)

        def backward(i, q, ctx, lse, gctx):
            return attention_bwd(scal_c[i], q, gctx, ctx, lse, cos_c[i], sin_c[i], row_c[i], k_all, kt_all, v_all)

        ctx_m, lse_m = forward(0, q_m)
        ctx_rm = to_chip(ctx_m)
        q_p, ctx_m = lax.optimization_barrier((q_p, ctx_m))
        ctx_p, lse_p = forward(1, q_p)
        ctx_rp = to_chip(ctx_p)
        ctx_o = to_core(ctx_p)
        q_m, ctx_m, ctx_p = lax.optimization_barrier((q_m, ctx_m, ctx_p))
        dq_m, dk_m, dv_m = backward(0, q_m, ctx_m, lse_m, gctx_m)
        q_p, dq_m = lax.optimization_barrier((q_p, dq_m))
        dq_p, dk_p, dv_p = backward(1, q_p, ctx_p, lse_p, gctx_p)

        two = 2 * n_rows
        d_kv = jnp.concatenate([dk_m + dk_p, dv_m + dv_p], axis=1)
        d_kv_mine = lax.dynamic_slice(d_kv, (chip * two, 0), (two, 2 * HEAD_DIM))
        d_kv_sent = lax.dynamic_slice(d_kv, ((1 - chip) * two, 0), (two, 2 * HEAD_DIM))
        d_kv_got = to_earlier(d_kv_sent)
        d_kv_sent, go_rm, norm_rm = lax.optimization_barrier((d_kv_sent, go_rm, norm_rm))
        dq_rm = to_chip(dq_m)
        dq_rp = to_chip(dq_p)
        dq_o = to_core(dq_p)
        go_rp = to_core(go_rm)
        norm_rp = to_core(norm_rm)

        no_place = jnp.zeros((2,), jnp.int32)
        bm, bn = 512, 2048
        wout_own, = weight_grad((ctx_m, ctx_p), (grad_out, go_p), None, no_place, None, 0, hid_width, bm, bn, 512)
        wq_own, = weight_grad((normed, normed_p), (dq_m, dq_p), None, no_place, None, 0, half, bm, bn, 512)

        def both_halves(mine, other):
            first = jnp.where(core == 0, mine, other)
            second = jnp.where(core == 0, other, mine)
            return jnp.concatenate([first, second], axis=-1)

        ctx_full = both_halves(ctx_m, ctx_o)
        y_out = (hid_f32 + jnp.dot(ctx_full, w_out, preferred_element_type=jnp.float32)).astype(jnp.bfloat16)

        ctx_rm, ctx_rp, go_rp, y_out, wq_own = lax.optimization_barrier((ctx_rm, ctx_rp, go_rp, y_out, wq_own))
        mine_o = jnp.stack([core * (half // bm), jnp.int32(0)]).astype(jnp.int32)
        other_o = jnp.stack([(1 - core) * (half // bm), jnp.int32(0)]).astype(jnp.int32)
        wout_half, wout_full = weight_grad((ctx_rm, ctx_rp), (go_rm, go_rp), wout_own, mine_o, (att_width, hid_width), 0, hid_width,
                                           bm, bn // 2, 512)
        wout_other = to_core(wout_half)

        d_kv = d_kv_mine + d_kv_got
        d_key = d_kv[:, :HEAD_DIM] * (HEAD_DIM ** -0.5)
        cos_k = lax.dynamic_slice(cos_all, (chip * two, 0), (two, HEAD_DIM))
        sin_k = lax.dynamic_slice(sin_all, (chip * two, 0), (two, HEAD_DIM))
        d_key = d_key * cos_k - swap_lanes(d_key) * sin_k
        d_kv = jnp.concatenate([d_key, d_kv[:, HEAD_DIM:]], axis=1).astype(jnp.bfloat16)
        d_kv_r = to_chip(d_kv)

        def pair_of(arr):
            return [lax.dynamic_slice(arr, (c * n_rows, 0), (n_rows, 2 * HEAD_DIM)) for c in (core, 1 - core)]

        dkv_m, dkv_p = pair_of(d_kv)
        dkv_o = to_core(dkv_p)
        grad_qkv = jnp.concatenate([both_halves(dq_m, dq_o),
                                    both_halves(dkv_m[:, :HEAD_DIM], dkv_o[:, :HEAD_DIM]),
                                    both_halves(dkv_m[:, HEAD_DIM:], dkv_o[:, HEAD_DIM:])], axis=1)
        grad_normed = lax.dot_general(grad_qkv, w_qkv, NT, preferred_element_type=jnp.float32)
        grad_gain = jnp.sum(grad_normed * x_hat, axis=0)
        scaled = grad_normed * gain_f32
        grad_hidden = (grad_out.astype(jnp.float32) + inv_rms * (scaled - x_hat * jnp.mean(scaled * x_hat, axis=-1, keepdims=True))).astype(jnp.bfloat16)
        kv_own, = weight_grad((normed, normed_p), (dkv_m, dkv_p), None, no_place, None, 0, 2 * HEAD_DIM, 1024, 2 * HEAD_DIM, 256)
        grad_wout = place_block(wout_full, wout_other, other_o, 512, 2048)

        def col_sums(first, second):
            return jnp.sum(first.astype(jnp.float32), axis=0) + jnp.sum(second.astype(jnp.float32), axis=0)

        own_sums = jnp.concatenate([col_sums(dq_m, dq_p), col_sums(dkv_m, dkv_p)])
        (dq_rm, dq_rp, norm_rm, norm_rp, grad_hidden, kv_own, own_sums, grad_wout) = lax.optimization_barrier(
            (dq_rm, dq_rp, norm_rm, norm_rp, grad_hidden, kv_own, own_sums, grad_wout))
        n_rem = (norm_rm, norm_rp)
        bn_q = half // 2
        grad_wqkv, sent = w_qkv.shape, []
        for part in range(2):
            mine_q = jnp.stack([jnp.int32(0), core * 2 + part]).astype(jnp.int32)
            other_q = jnp.stack([jnp.int32(0), (1 - core) * 2 + part]).astype(jnp.int32)
            got, grad_wqkv = weight_grad(n_rem, (dq_rm, dq_rp), wq_own, mine_q, grad_wqkv, part * bn_q, bn_q, bm, bn_q, 512)
            sent.append((to_core(got), other_q))
        d_kv_r, grad_wqkv = lax.optimization_barrier((d_kv_r, grad_wqkv))
        dkv_r = pair_of(d_kv_r)
        kv_half, = weight_grad(n_rem, dkv_r, kv_own, no_place, None, 0, 2 * HEAD_DIM, 1024, 2 * HEAD_DIM, 256)
        kv_other = to_core(kv_half)
        for got, other_q in sent:
            grad_wqkv = place_block(grad_wqkv, got, other_q, 512, bn_q)
        kv_cols = jnp.concatenate([both_halves(kv_half[:, :HEAD_DIM], kv_other[:, :HEAD_DIM]),
                                   both_halves(kv_half[:, HEAD_DIM:], kv_other[:, HEAD_DIM:])], axis=1)
        grad_wqkv = lax.dynamic_update_slice(grad_wqkv, kv_cols, (0, att_width))

        b_half = own_sums + to_chip(own_sums)
        b_other = to_core(b_half)
        grad_bqkv = jnp.concatenate([both_halves(b_half[:half], b_other[:half]),
                                     both_halves(b_half[half:half + HEAD_DIM], b_other[half:half + HEAD_DIM]),
                                     both_halves(b_half[half + HEAD_DIM:], b_other[half + HEAD_DIM:])])
        grad_gain = grad_gain + to_core(grad_gain)
        grad_gain = grad_gain + to_chip(grad_gain)
        return y_out, grad_hidden, grad_gain, grad_wqkv, grad_bqkv, grad_wout

    act_spec = P(('dp', 'cp'), None)
    row_spec = P(('dp', 'cp'))
    return jax.shard_map(layer, mesh=mesh,
                         in_specs=(act_spec, row_spec, row_spec, P(), P(), P(), P(), act_spec),
                         out_specs=(act_spec, act_spec, P('dp'), P('dp', None), P('dp'), P('dp', None)),
                         check_vma=False)
```

```python
import functools

import jax
import jax.numpy as jnp
from jax import lax
from jax.experimental import pallas as pl
from jax.experimental.pallas import tpu as pltpu
from jax.sharding import PartitionSpec as P

HEAD_DIM = 128
ROT_DIMS = 64
ROPE_BASE = 5000000.0
EPS_NORM = 1e-5
NEG_BIG = -1e30
LOG2E = 1.4426950408889634
BQ = 256
BK = 256
VMEM_LIMIT = 60 * 1024 * 1024


NT = (((1,), (1,)), ((), ()))
NN = (((1,), (0,)), ((), ()))
TN = (((0,), (0,)), ((), ()))


def dotf(a, b, dims):
    return lax.dot_general(a, b, dims, preferred_element_type=jnp.float32)


def pair_swap(values):
    lane = lax.broadcasted_iota(jnp.int32, values.shape, 1)
    return jnp.where(lane % 2 == 0, pltpu.roll(values, HEAD_DIM - 1, 1), pltpu.roll(values, 1, 1))


def load_rotated(q_ref, cos_ref, sin_ref, qs_ref, n_heads):
    cos_t = cos_ref[...]
    sin_t = sin_ref[...]
    for h in range(n_heads):
        val = q_ref[:, h * HEAD_DIM:(h + 1) * HEAD_DIM].astype(jnp.float32)
        qs_ref[h * BQ:(h + 1) * BQ, :] = (val * cos_t + pair_swap(val) * sin_t).astype(jnp.bfloat16)


def visible(start_row, kv, q_base):
    k_idx = kv * BK + lax.broadcasted_iota(jnp.int32, (BK, BQ), 0)
    q_idx = q_base + lax.broadcasted_iota(jnp.int32, (BK, BQ), 1)
    return (k_idx >= start_row) & (k_idx <= q_idx)


def mask_heads(s_t, start_row, kv, q_base, n_heads):
    vis = visible(start_row, kv, q_base)
    return jnp.concatenate([jnp.where(vis, s_t[:, h * BQ:(h + 1) * BQ], NEG_BIG) for h in range(n_heads)], axis=1)


def fwd_kernel(n_heads, sc_ref, q_ref, cos_ref, sin_ref, start_ref, k_ref, vt_ref,
               ctx_ref, lse_ref, qs_ref, acc_ref):
    i = pl.program_id(0)
    q_base = sc_ref[0] + i * BQ
    lo = sc_ref[1 + 2 * i]
    full_lo = sc_ref[2 + 2 * i]
    diag = q_base // BK
    scale = HEAD_DIM ** -0.5 * LOG2E
    load_rotated(q_ref, cos_ref, sin_ref, qs_ref, n_heads)
    start_row = start_ref[...]
    acc_ref[...] = jnp.zeros_like(acc_ref)

    def step(masked, kv, carry):
        m_run, l_run = carry
        k_off = pl.multiple_of(kv * BK, BK)
        s_t = dotf(k_ref[pl.ds(k_off, BK), :], qs_ref[...], NT) * scale
        if masked:
            s_t = mask_heads(s_t, start_row, kv, q_base, n_heads)
        m_new = jnp.maximum(m_run, jnp.max(s_t, axis=0, keepdims=True))
        p_t = jnp.exp2(s_t - m_new)
        rescale = jnp.exp2(m_run - m_new)
        l_new = l_run * rescale + jnp.sum(p_t, axis=0, keepdims=True)
        acc_ref[...] = acc_ref[...] * rescale + dotf(vt_ref[:, pl.ds(k_off, BK)], p_t.astype(jnp.bfloat16), NN)
        return m_new, l_new

    carry = (jnp.full((1, n_heads * BQ), NEG_BIG, jnp.float32), jnp.zeros((1, n_heads * BQ), jnp.float32))
    carry = lax.fori_loop(lo, full_lo, functools.partial(step, True), carry)
    carry = lax.fori_loop(full_lo, diag, functools.partial(step, False), carry)
    m_run, l_run = step(True, diag, carry)
    lse = m_run + jnp.log2(l_run)
    for h in range(n_heads):
        span = slice(h * BQ, (h + 1) * BQ)
        o_t = acc_ref[:, span] / l_run[:, span]
        ctx_ref[:, h * HEAD_DIM:(h + 1) * HEAD_DIM] = o_t.T.astype(jnp.bfloat16)
        lse_ref[h:h + 1, :] = lse[:, span]


def bwd_kernel(n_heads, sc_ref, q_ref, do_ref, ctx_ref, lse_ref, cos_ref, sin_ref, start_ref,
               k_ref, kt_ref, v_ref, dq_ref, dk_ref, dv_ref, qs_ref, ds_ref, rd_ref, dqt_ref):
    i = pl.program_id(0)
    q_base = sc_ref[0] + i * BQ
    lo = sc_ref[1 + 2 * i]
    full_lo = sc_ref[2 + 2 * i]
    diag = q_base // BK
    factor = HEAD_DIM ** -0.5
    scale = factor * LOG2E

    @pl.when(i == 0)
    def _():
        dk_ref[...] = jnp.zeros_like(dk_ref)
        dv_ref[...] = jnp.zeros_like(dv_ref)

    load_rotated(q_ref, cos_ref, sin_ref, qs_ref, n_heads)
    for h in range(n_heads):
        cols = slice(h * HEAD_DIM, (h + 1) * HEAD_DIM)
        do_h = do_ref[:, cols]
        ds_ref[h * BQ:(h + 1) * BQ, :] = do_h
        prod = do_h.astype(jnp.float32) * ctx_ref[:, cols].astype(jnp.float32)
        span = slice(h * BQ, (h + 1) * BQ)
        rd_ref[0:1, span] = jnp.sum(prod.T, axis=0, keepdims=True)
        rd_ref[1:2, span] = lse_ref[h:h + 1, :]
    start_row = start_ref[...]
    cos_t = cos_ref[...]
    sin_t = sin_ref[...]
    dqt_ref[...] = jnp.zeros_like(dqt_ref)
    row_dot = rd_ref[0:1, :]
    log_norm = rd_ref[1:2, :]

    def step(masked, kv, _):
        k_off = pl.multiple_of(kv * BK, BK)
        keys = pl.ds(k_off, BK)
        s_t = dotf(k_ref[keys, :], qs_ref[...], NT) * scale
        if masked:
            s_t = mask_heads(s_t, start_row, kv, q_base, n_heads)
        p_t = jnp.exp2(s_t - log_norm)
        g_t = (p_t * (dotf(v_ref[keys, :], ds_ref[...], NT) - row_dot)).astype(jnp.bfloat16)
        dqt_ref[...] += dotf(kt_ref[:, keys], g_t, NN)
        dv_ref[keys, :] += dotf(p_t.astype(jnp.bfloat16), ds_ref[...], NN)
        dk_ref[keys, :] += dotf(g_t, qs_ref[...], NN)
        return 0

    lax.fori_loop(lo, full_lo, functools.partial(step, True), 0)
    lax.fori_loop(full_lo, diag, functools.partial(step, False), 0)
    step(True, diag, 0)
    for h in range(n_heads):
        dq_h = dqt_ref[:, h * BQ:(h + 1) * BQ].T * factor
        dq_ref[:, h * HEAD_DIM:(h + 1) * HEAD_DIM] = (dq_h * cos_t - pair_swap(dq_h) * sin_t).astype(jnp.bfloat16)


def attn_cost(n_rows, width, n_dots):
    return pl.CostEstimate(flops=int(n_dots * 4 * n_rows * 1400 * width), bytes_accessed=3 * n_rows * width * 2,
                           transcendentals=0)


def attention_fwd(scal, q_pre, cos_t, sin_t, start_row, k_all, vt_all):
    n_rows, width = q_pre.shape
    n_heads = width // HEAD_DIM
    n_keys = k_all.shape[0]
    row_blk = lambda i, sc: (i, 0)
    lane_blk = lambda i, sc: (0, i)
    whole = lambda i, sc: (0, 0)
    return pl.pallas_call(
        functools.partial(fwd_kernel, n_heads),
        grid_spec=pltpu.PrefetchScalarGridSpec(
            num_scalar_prefetch=1, grid=(n_rows // BQ,),
            in_specs=[pl.BlockSpec((BQ, width), row_blk), pl.BlockSpec((BQ, HEAD_DIM), row_blk),
                      pl.BlockSpec((BQ, HEAD_DIM), row_blk), pl.BlockSpec((1, BQ), lane_blk),
                      pl.BlockSpec((n_keys, HEAD_DIM), whole), pl.BlockSpec((HEAD_DIM, n_keys), whole)],
            out_specs=[pl.BlockSpec((BQ, width), row_blk), pl.BlockSpec((n_heads, BQ), lane_blk)],
            scratch_shapes=[pltpu.VMEM((n_heads * BQ, HEAD_DIM), jnp.bfloat16),
                            pltpu.VMEM((HEAD_DIM, n_heads * BQ), jnp.float32)]),
        out_shape=[jax.ShapeDtypeStruct((n_rows, width), jnp.bfloat16), jax.ShapeDtypeStruct((n_heads, n_rows), jnp.float32)],
        compiler_params=pltpu.CompilerParams(dimension_semantics=("arbitrary",), vmem_limit_bytes=VMEM_LIMIT),
        cost_estimate=attn_cost(n_rows, width, 1), name="attn_fwd",
    )(scal, q_pre, cos_t, sin_t, start_row, k_all, vt_all)


def attention_bwd(scal, q_pre, grad_ctx, ctx, lse, cos_t, sin_t, start_row, k_all, kt_all, v_all):
    n_rows, width = q_pre.shape
    n_heads = width // HEAD_DIM
    n_keys = k_all.shape[0]
    row_blk = lambda i, sc: (i, 0)
    lane_blk = lambda i, sc: (0, i)
    whole = lambda i, sc: (0, 0)
    wide = pl.BlockSpec((BQ, width), row_blk)
    kv_spec = pl.BlockSpec((n_keys, HEAD_DIM), whole)
    return pl.pallas_call(
        functools.partial(bwd_kernel, n_heads),
        grid_spec=pltpu.PrefetchScalarGridSpec(
            num_scalar_prefetch=1, grid=(n_rows // BQ,),
            in_specs=[wide, wide, wide, pl.BlockSpec((n_heads, BQ), lane_blk), pl.BlockSpec((BQ, HEAD_DIM), row_blk),
                      pl.BlockSpec((BQ, HEAD_DIM), row_blk), pl.BlockSpec((1, BQ), lane_blk),
                      kv_spec, pl.BlockSpec((HEAD_DIM, n_keys), whole), kv_spec],
            out_specs=[wide, kv_spec, kv_spec],
            scratch_shapes=[pltpu.VMEM((n_heads * BQ, HEAD_DIM), jnp.bfloat16),
                            pltpu.VMEM((n_heads * BQ, HEAD_DIM), jnp.bfloat16),
                            pltpu.VMEM((2, n_heads * BQ), jnp.float32),
                            pltpu.VMEM((HEAD_DIM, n_heads * BQ), jnp.float32)]),
        out_shape=[jax.ShapeDtypeStruct((n_rows, width), jnp.bfloat16)] + [jax.ShapeDtypeStruct((n_keys, HEAD_DIM), jnp.float32)] * 2,
        compiler_params=pltpu.CompilerParams(dimension_semantics=("arbitrary",), vmem_limit_bytes=VMEM_LIMIT),
        cost_estimate=attn_cost(n_rows, width, 2.5), name="attn_bwd",
    )(scal, q_pre, grad_ctx, ctx, lse, cos_t, sin_t, start_row, k_all, kt_all, v_all)


def wgrad_kernel(col_step, n_prev, n_out, sc_ref, *refs):
    a_refs, b_refs, refs = refs[:4], refs[4:8], refs[8:]
    out_refs = refs[-n_out:]
    width = out_refs[0].shape[1]

    def cols(j, _):
        span = pl.ds(pl.multiple_of(j * col_step, col_step), col_step)
        total = dotf(a_refs[0][...], b_refs[0][:, span], TN)
        for a_ref, b_ref in zip(a_refs[1:], b_refs[1:]):
            total += dotf(a_ref[...], b_ref[:, span], TN)
        if n_prev:
            total = refs[0][:, span] + total
        for out in out_refs:
            out[:, span] = total
        return 0

    lax.fori_loop(0, width // col_step, cols, 0)


def weight_grad(a_pair, b_pair, prev, place, full, col0, n_dim, bm, bn, col_step):
    n_tok, m_dim = a_pair[0].shape
    blk0 = col0 // bn

    def piece(val, side):
        first, second = val if isinstance(val, tuple) else (val, val)
        shape = (n_tok // 2, bm if side == 0 else bn)
        specs = []
        for row in (0, 0 if isinstance(val, tuple) else 1):
            index = (lambda n, m, sc, row=row: (row, m)) if side == 0 else (lambda n, m, sc, row=row: (row, n + blk0))
            specs.append(pl.BlockSpec(shape, index))
        return [first, second], specs

    in_specs, args = [], []
    for side, pair in enumerate((a_pair, b_pair)):
        for val in pair:
            arrs, specs = piece(val, side)
            args += arrs
            in_specs += specs
    if prev is not None:
        in_specs.append(pl.BlockSpec((bm, bn), lambda n, m, sc: (m, n + blk0)))
        args.append(prev)
    out_specs = [pl.BlockSpec((bm, bn), lambda n, m, sc: (m, n))]
    out_shape = [jax.ShapeDtypeStruct((m_dim, n_dim), jnp.float32)]
    aliases = {}
    if full is not None:
        shape = full if isinstance(full, tuple) else full.shape
        out_specs.append(pl.BlockSpec((bm, bn), lambda n, m, sc: (sc[0] + m, sc[1] + n)))
        out_shape.append(jax.ShapeDtypeStruct(shape, jnp.float32))
        if not isinstance(full, tuple):
            in_specs.append(pl.BlockSpec(memory_space=pl.ANY))
            args.append(full)
            aliases = {len(args): 1}
    return pl.pallas_call(
        functools.partial(wgrad_kernel, col_step, prev is not None, len(out_shape)),
        grid_spec=pltpu.PrefetchScalarGridSpec(num_scalar_prefetch=1, grid=(n_dim // bn, m_dim // bm),
                                               in_specs=in_specs, out_specs=out_specs),
        out_shape=out_shape, input_output_aliases=aliases,
        compiler_params=pltpu.CompilerParams(dimension_semantics=("arbitrary", "arbitrary"), vmem_limit_bytes=VMEM_LIMIT),
        cost_estimate=pl.CostEstimate(flops=4 * n_tok * m_dim * n_dim, transcendentals=0,
                                      bytes_accessed=m_dim * n_dim * 8 + 4 * n_tok * (m_dim + n_dim)),
    )(place, *args)


def place_kernel(sc_ref, src_ref, full_ref, out_ref):
    out_ref[...] = src_ref[...]


def place_block(full, block, place, bm, bn):
    m_dim, n_dim = block.shape
    return pl.pallas_call(
        place_kernel,
        grid_spec=pltpu.PrefetchScalarGridSpec(
            num_scalar_prefetch=1, grid=(m_dim // bm, n_dim // bn),
            in_specs=[pl.BlockSpec((bm, bn), lambda m, n, sc: (m, n)), pl.BlockSpec(memory_space=pl.ANY)],
            out_specs=pl.BlockSpec((bm, bn), lambda m, n, sc: (sc[0] + m, sc[1] + n))),
        out_shape=jax.ShapeDtypeStruct(full.shape, full.dtype),
        input_output_aliases={2: 0},
        compiler_params=pltpu.CompilerParams(dimension_semantics=("arbitrary", "arbitrary"), vmem_limit_bytes=VMEM_LIMIT),
        cost_estimate=pl.CostEstimate(flops=0, transcendentals=0, bytes_accessed=8 * m_dim * n_dim),
    )(place, block, full)


def swap_lanes(values):
    lane = lax.broadcasted_iota(jnp.int32, values.shape, values.ndim - 1)
    return jnp.where(lane % 2 == 0, jnp.roll(values, -1, axis=-1), jnp.roll(values, 1, axis=-1))


def solution(mesh):
    core_swap = [(0, 1), (1, 0), (2, 3), (3, 2)]
    chip_swap = [(0, 2), (2, 0), (1, 3), (3, 1)]

    def to_core(val):
        return lax.ppermute(val, 'cp', core_swap)

    def to_chip(val):
        return lax.ppermute(val, 'cp', chip_swap)

    def to_later(val):
        return lax.ppermute(val, 'cp', [(0, 2), (1, 3)])

    def to_earlier(val):
        return lax.ppermute(val, 'cp', [(2, 0), (3, 1)])

    def layer(hidden, seg_id, doc_pos, norm_gain, w_qkv, b_qkv, w_out, grad_out):
        n_rows, hid_width = hidden.shape
        att_width = w_out.shape[0]
        half = att_width // 2
        idx = lax.axis_index('cp')
        core = idx % 2
        chip = idx // 2
        chunk_ids = (idx, idx ^ 1, idx ^ 2, idx ^ 3)

        pos_all = lax.all_gather(doc_pos, 'cp', axis=0, tiled=True)
        hidden, grad_out, pos_all = lax.optimization_barrier((hidden, grad_out, pos_all))

        go_ra = to_chip(grad_out[:n_rows // 2])
        hid_f32 = hidden.astype(jnp.float32)
        inv_rms = lax.rsqrt(jnp.mean(hid_f32 * hid_f32, axis=-1, keepdims=True) + EPS_NORM)
        x_hat = hid_f32 * inv_rms
        gain_f32 = norm_gain.astype(jnp.float32)
        normed = (x_hat * gain_f32).astype(jnp.bfloat16)
        normed_p = to_core(normed)
        go_p = to_core(grad_out)

        n_seq = pos_all.shape[0]
        starts = jnp.arange(n_seq, dtype=jnp.int32) - pos_all
        lane = jnp.arange(HEAD_DIM)
        exponent = -((lane // 2) * 2).astype(jnp.float32) / ROT_DIMS
        inv_freq = ROPE_BASE ** exponent
        angles = pos_all.astype(jnp.float32)[:, None] * inv_freq[None, :]
        turned = (lane < ROT_DIMS)[None, :]
        cos_all = jnp.where(turned, jnp.cos(angles), 1.0)
        sin_all = jnp.where(turned, jnp.sin(angles) * jnp.where(lane % 2 == 0, -1.0, 1.0)[None, :], 0.0)

        def chunk_of(arr, g, axis=0):
            return lax.dynamic_slice_in_dim(arr, g * n_rows, n_rows, axis)

        cos_c = [chunk_of(cos_all, g) for g in chunk_ids]
        sin_c = [chunk_of(sin_all, g) for g in chunk_ids]
        start_c = [chunk_of(starts, g) for g in chunk_ids]
        scal_c = []
        for g, st in zip(chunk_ids, start_c):
            diag = (g * n_rows) // BK + jnp.arange(n_rows // BQ, dtype=jnp.int32) * (BQ // BK)
            lo = st[::BQ] // BK
            full_lo = jnp.minimum((st[BQ - 1::BQ] + BK - 1) // BK, diag)
            lo = jnp.minimum(lo, full_lo)
            scal_c.append(jnp.concatenate([(g * n_rows)[None], jnp.stack([lo, full_lo], axis=1).reshape(-1)]).astype(jnp.int32))
        row_c = [st[None, :] for st in start_c]

        wq = lax.dynamic_slice(w_qkv, (0, core * half), (hid_width, half))
        wk = lax.dynamic_slice(w_qkv, (0, att_width + core * HEAD_DIM), (hid_width, HEAD_DIM))
        wv = lax.dynamic_slice(w_qkv, (0, att_width + (2 + core) * HEAD_DIM), (hid_width, HEAD_DIM))
        wkv = jnp.concatenate([wk, wv], axis=1)
        b_f32 = b_qkv.astype(jnp.float32)
        bq = lax.dynamic_slice(b_f32, (core * half,), (half,))
        bkv = jnp.concatenate([lax.dynamic_slice(b_f32, (att_width + core * HEAD_DIM,), (HEAD_DIM,)),
                               lax.dynamic_slice(b_f32, (att_width + (2 + core) * HEAD_DIM,), (HEAD_DIM,))])
        wo = lax.dynamic_slice(w_out, (core * half, 0), (half, hid_width))

        def project(act, wgt, bias):
            return (jnp.dot(act, wgt, preferred_element_type=jnp.float32) + bias).astype(jnp.bfloat16)

        def project_kv(act, i):
            kv = project(act, wkv, bkv)
            k_f32 = kv[:, :HEAD_DIM].astype(jnp.float32)
            k_rot = (k_f32 * cos_c[i] + swap_lanes(k_f32) * sin_c[i]).astype(jnp.bfloat16)
            return jnp.concatenate([k_rot, kv[:, HEAD_DIM:]], axis=1)

        kv_m = project_kv(normed, 0)
        kv_rm = to_later(kv_m)
        kv_p = project_kv(normed_p, 1)
        kv_rp = to_later(kv_p)
        go_rb = to_chip(grad_out[n_rows // 2:])
        norm_rm = to_chip(normed)
        q_m = project(normed, wq, bq)
        q_p = project(normed_p, wq, bq)

        def grad_context(go):
            return lax.dot_general(go, wo, NT, preferred_element_type=jnp.float32).astype(jnp.bfloat16)

        gctx_m, gctx_p = grad_context(grad_out), grad_context(go_p)
        kv_rm, kv_rp, q_m, q_p, gctx_m, gctx_p = lax.optimization_barrier((kv_rm, kv_rp, q_m, q_p, gctx_m, gctx_p))
        kv_all = jnp.zeros((n_seq, 2 * HEAD_DIM), jnp.bfloat16)
        for g, kv in zip(chunk_ids, (kv_m, kv_p, kv_rm, kv_rp)):
            kv_all = lax.dynamic_update_slice(kv_all, kv, (g * n_rows, 0))
        k_all, v_all = kv_all[:, :HEAD_DIM], kv_all[:, HEAD_DIM:]
        kt_all, vt_all = k_all.T, v_all.T

        def forward(i, q):
            return attention_fwd(scal_c[i], q, cos_c[i], sin_c[i], row_c[i], k_all, vt_all)

        def backward(i, q, ctx, lse, gctx):
            return attention_bwd(scal_c[i], q, gctx, ctx, lse, cos_c[i], sin_c[i], row_c[i], k_all, kt_all, v_all)

        ctx_m, lse_m = forward(0, q_m)
        ctx_rm = to_chip(ctx_m)
        q_p, ctx_m = lax.optimization_barrier((q_p, ctx_m))
        ctx_p, lse_p = forward(1, q_p)
        ctx_rp = to_chip(ctx_p)
        ctx_o = to_core(ctx_p)
        q_m, ctx_m, ctx_p = lax.optimization_barrier((q_m, ctx_m, ctx_p))
        dq_m, dk_m, dv_m = backward(0, q_m, ctx_m, lse_m, gctx_m)
        q_p, dq_m = lax.optimization_barrier((q_p, dq_m))
        dq_p, dk_p, dv_p = backward(1, q_p, ctx_p, lse_p, gctx_p)

        two = 2 * n_rows
        d_kv = jnp.concatenate([dk_m + dk_p, dv_m + dv_p], axis=1)
        d_kv_mine = lax.dynamic_slice(d_kv, (chip * two, 0), (two, 2 * HEAD_DIM))
        d_kv_sent = lax.dynamic_slice(d_kv, ((1 - chip) * two, 0), (two, 2 * HEAD_DIM))
        d_kv_got = to_earlier(d_kv_sent)
        d_kv_sent, go_ra, go_rb, norm_rm = lax.optimization_barrier((d_kv_sent, go_ra, go_rb, norm_rm))
        dq_rm = to_chip(dq_m)
        dq_rp = to_chip(dq_p)
        dq_o = to_core(dq_p)
        go_rm = (go_ra, go_rb)
        go_rp = (to_core(go_ra), to_core(go_rb))
        norm_rp = to_core(norm_rm)

        no_place = jnp.zeros((2,), jnp.int32)
        bm, bn = 512, 2048
        wout_own, = weight_grad((ctx_m, ctx_p), (grad_out, go_p), None, no_place, None, 0, hid_width, bm, bn, 512)
        wq_own, = weight_grad((normed, normed_p), (dq_m, dq_p), None, no_place, None, 0, half, bm, bn, 512)

        def both_halves(mine, other):
            first = jnp.where(core == 0, mine, other)
            second = jnp.where(core == 0, other, mine)
            return jnp.concatenate([first, second], axis=-1)

        ctx_full = both_halves(ctx_m, ctx_o)
        y_out = (hid_f32 + jnp.dot(ctx_full, w_out, preferred_element_type=jnp.float32)).astype(jnp.bfloat16)

        ctx_rm, ctx_rp, go_rp, y_out, wq_own = lax.optimization_barrier((ctx_rm, ctx_rp, go_rp, y_out, wq_own))
        mine_o = jnp.stack([core * (half // bm), jnp.int32(0)]).astype(jnp.int32)
        other_o = jnp.stack([(1 - core) * (half // bm), jnp.int32(0)]).astype(jnp.int32)
        wout_half, wout_full = weight_grad((ctx_rm, ctx_rp), (go_rm, go_rp), wout_own, mine_o, (att_width, hid_width), 0, hid_width,
                                           bm, bn, 512)
        wout_half, d_kv_got = lax.optimization_barrier((wout_half, d_kv_got))
        wout_other = to_core(wout_half)

        d_kv = d_kv_mine + d_kv_got
        d_key = d_kv[:, :HEAD_DIM] * (HEAD_DIM ** -0.5)
        cos_k = lax.dynamic_slice(cos_all, (chip * two, 0), (two, HEAD_DIM))
        sin_k = lax.dynamic_slice(sin_all, (chip * two, 0), (two, HEAD_DIM))
        d_key = d_key * cos_k - swap_lanes(d_key) * sin_k
        d_kv = jnp.concatenate([d_key, d_kv[:, HEAD_DIM:]], axis=1).astype(jnp.bfloat16)
        d_kv_r = to_chip(d_kv)

        def pair_of(arr):
            return [lax.dynamic_slice(arr, (c * n_rows, 0), (n_rows, 2 * HEAD_DIM)) for c in (core, 1 - core)]

        dkv_m, dkv_p = pair_of(d_kv)
        dkv_o = to_core(dkv_p)
        grad_qkv = jnp.concatenate([both_halves(dq_m, dq_o),
                                    both_halves(dkv_m[:, :HEAD_DIM], dkv_o[:, :HEAD_DIM]),
                                    both_halves(dkv_m[:, HEAD_DIM:], dkv_o[:, HEAD_DIM:])], axis=1)
        grad_normed = lax.dot_general(grad_qkv, w_qkv, NT, preferred_element_type=jnp.float32)
        grad_gain = jnp.sum(grad_normed * x_hat, axis=0)
        scaled = grad_normed * gain_f32
        grad_hidden = (grad_out.astype(jnp.float32) + inv_rms * (scaled - x_hat * jnp.mean(scaled * x_hat, axis=-1, keepdims=True))).astype(jnp.bfloat16)
        kv_own, = weight_grad((normed, normed_p), (dkv_m, dkv_p), None, no_place, None, 0, 2 * HEAD_DIM, 1024, 2 * HEAD_DIM, 256)
        grad_wout = place_block(wout_full, wout_other, other_o, 512, 2048)

        def col_sums(first, second):
            return jnp.sum(first.astype(jnp.float32), axis=0) + jnp.sum(second.astype(jnp.float32), axis=0)

        own_sums = jnp.concatenate([col_sums(dq_m, dq_p), col_sums(dkv_m, dkv_p)])
        (dq_rm, dq_rp, norm_rm, norm_rp, grad_hidden, kv_own, own_sums, grad_wout) = lax.optimization_barrier(
            (dq_rm, dq_rp, norm_rm, norm_rp, grad_hidden, kv_own, own_sums, grad_wout))
        n_rem = (norm_rm, norm_rp)
        bn_q = half // 2
        grad_wqkv, sent = w_qkv.shape, []
        for part in range(2):
            mine_q = jnp.stack([jnp.int32(0), core * 2 + part]).astype(jnp.int32)
            other_q = jnp.stack([jnp.int32(0), (1 - core) * 2 + part]).astype(jnp.int32)
            got, grad_wqkv = weight_grad(n_rem, (dq_rm, dq_rp), wq_own, mine_q, grad_wqkv, part * bn_q, bn_q, bm, bn_q, 512)
            sent.append((to_core(got), other_q))
            if part == 0:
                d_kv_r, grad_wqkv = lax.optimization_barrier((d_kv_r, grad_wqkv))
                dkv_r = pair_of(d_kv_r)
                kv_half, = weight_grad(n_rem, dkv_r, kv_own, no_place, None, 0, 2 * HEAD_DIM, 1024, 2 * HEAD_DIM, 256)
                kv_other = to_core(kv_half)
        for got, other_q in sent:
            grad_wqkv = place_block(grad_wqkv, got, other_q, 512, bn_q)
        kv_cols = jnp.concatenate([both_halves(kv_half[:, :HEAD_DIM], kv_other[:, :HEAD_DIM]),
                                   both_halves(kv_half[:, HEAD_DIM:], kv_other[:, HEAD_DIM:])], axis=1)
        grad_wqkv = lax.dynamic_update_slice(grad_wqkv, kv_cols, (0, att_width))

        b_half = own_sums + to_chip(own_sums)
        b_other = to_core(b_half)
        grad_bqkv = jnp.concatenate([both_halves(b_half[:half], b_other[:half]),
                                     both_halves(b_half[half:half + HEAD_DIM], b_other[half:half + HEAD_DIM]),
                                     both_halves(b_half[half + HEAD_DIM:], b_other[half + HEAD_DIM:])])
        grad_gain = grad_gain + to_core(grad_gain)
        grad_gain = grad_gain + to_chip(grad_gain)
        return y_out, grad_hidden, grad_gain, grad_wqkv, grad_bqkv, grad_wout

    act_spec = P(('dp', 'cp'), None)
    row_spec = P(('dp', 'cp'))
    return jax.shard_map(layer, mesh=mesh,
                         in_specs=(act_spec, row_spec, row_spec, P(), P(), P(), P(), act_spec),
                         out_specs=(act_spec, act_spec, P('dp'), P('dp', None), P('dp'), P('dp', None)),
                         check_vma=False)
```
